32 devices in a mesh: row: 8 (over y, x, core), col: 4 (over z).
Axes of the slice: x: 2, y: 2, z: 4, core: 2. Of those that a mesh axis runs over, the one named last changes fastest.
Arguments:
- surface_height: float32 [2048, 2048], P('row', 'col'), may hold values from -1.2 to 1.2
- surface_potential: float32 [2048, 2048], P('row', 'col'), may hold values from -4 to 4
- velocity: float32 [3, 16, 1024, 1024], P(None, None, 'row', 'col'), may hold values from -1.25 to 1.25
Outputs:
- height_rate: float32 [2048, 2048], P('row', 'col')
- potential_rate: float32 [2048, 2048], P('row', 'col')
- velocity_next: float32 [3, 16, 1024, 1024], P(None, None, 'row', 'col')
The draws below stay inside these ranges and needn't reach their ends.
All inputs are finite; a program needn't handle non-finite values.
Results may differ from the reference program's by a relative error of at most 0.00019.
Values sent between devices are 32-bit elements; how exact they have to be, the bound alone decides.
No kernel may reach another device: no remote copies, remote signals or barrier semaphores. Data moves between devices by JAX's collectives and lax.ppermute only.
A program may use at most 192 MiB of HBM per device.

```python
import jax
import jax.numpy as jnp

NX = 2048
NY = 2048
LZ = 16
COARSE = 2
LYALL = 1024
LXALL = 1024


def draw_surface_height(key, part):
    rough_key = jax.random.fold_in(jax.random.fold_in(key, 11), 0)
    return 0.3 * jnp.clip(jax.random.normal(rough_key, (NY, NX), jnp.float32), -4.0, 4.0)


def draw_surface_potential(key, part):
    rough_key = jax.random.fold_in(jax.random.fold_in(key, 23), 0)
    return jnp.clip(jax.random.normal(rough_key, (NY, NX), jnp.float32), -4.0, 4.0)


def block_levels(rng, dims, cuts, smallest, largest):
    def one(axis_at, parts):
        draws = jax.random.uniform(jax.random.fold_in(jax.random.fold_in(rng, 6), axis_at), (parts,), jnp.float32, smallest / len(cuts), largest / len(cuts))
        return jnp.repeat(jnp.exp(draws), dims[axis_at] // parts).reshape((-1,) + (1,) * (len(dims) - axis_at - 1))

    level = one(*cuts[0])
    for cut in cuts[1:]:
        level = level * one(*cut)
    return level


def noise(own_key, shape, deviation, limit, cuts=(), held_as=jnp.bfloat16):
    array = jax.random.normal(own_key, shape, jnp.float32) * deviation
    if len(cuts) > 0:
        array = block_levels(own_key, shape, cuts, -0.22, 0.18) * array
    return jnp.clip(array, min=-limit, max=limit).astype(held_as)


def setup_inputs(seed: int = 0) -> dict:
    arg_keys = jax.random.split(jax.random.key(seed), 4)
    return {
        "surface_height": draw_surface_height(jax.random.fold_in(arg_keys[3], 71), 0),
        "surface_potential": draw_surface_potential(jax.random.fold_in(arg_keys[3], 71), 0),
        "velocity": noise(arg_keys[2], (3, LZ, LYALL, LXALL), 0.2, 1.25, ((2, 8), (3, 4)), jnp.float32),
    }


GRAVITY = 1.0
SURFACE_STEP = 0.05
FLOW_STEP = 0.5
VISCOSITY = 0.2
DECAY_RATE = 0.05

def wave_numbers(index, length):
    signed = jnp.where(index < length // 2, index, index - length)
    kept_mask = (jnp.abs(signed) <= length // 3).astype(jnp.float32)
    return (2.0 * jnp.pi / length * signed.astype(jnp.float32), kept_mask)

def coarsen(source):
    rows_out = source.shape[0] // COARSE
    cols_out = source.shape[1] // COARSE
    return source.reshape(rows_out, COARSE, cols_out, COARSE).mean(axis=(1, 3))

def flow_update(padded_flow, padded_load, surface_u, surface_v):
    depth_count = padded_flow.shape[1]
    level_mid = jnp.arange(depth_count, dtype=jnp.float32)[:, None, None] + 0.5
    drift_decay = jnp.exp(-2.0 * DECAY_RATE * level_mid)
    load_decay = jnp.exp(-DECAY_RATE * level_mid)

    def derivs(source, top_value):
        middle = source[:, 1:-1, 1:-1]
        above_cell = jnp.concatenate([top_value[None], middle[:-1]], axis=0)
        below_cell = jnp.concatenate([middle[1:], middle[-1:]], axis=0)
        east_side = source[:, 1:-1, 2:]
        west_side = source[:, 1:-1, :-2]
        north_side = source[:, 2:, 1:-1]
        south_side = source[:, :-2, 1:-1]
        laplace = east_side + west_side + north_side + south_side + above_cell + below_cell - 6.0 * middle
        return (middle, 0.5 * (east_side - west_side), 0.5 * (north_side - south_side), 0.5 * (above_cell - below_cell), laplace)
    u_mid, u_dx, u_dy, u_dz, u_lap = derivs(padded_flow[0], surface_u)
    v_mid, v_dx, v_dy, v_dz, v_lap = derivs(padded_flow[1], surface_v)
    w_mid, w_dx, w_dy, w_dz, w_lap = derivs(padded_flow[2], jnp.zeros_like(surface_u))
    vort_x = w_dy - v_dz
    vort_y = u_dz - w_dx
    vort_z = v_dx - u_dy
    drift_u = surface_u[None] * drift_decay
    drift_v = surface_v[None] * drift_decay
    load_x = 0.5 * (padded_load[1:-1, 2:] - padded_load[1:-1, :-2])[None] * load_decay
    load_y = 0.5 * (padded_load[2:, 1:-1] - padded_load[:-2, 1:-1])[None] * load_decay

    def advance(middle, slope_x, slope_y, slope_z, laplace, forcing):
        carried = u_mid * slope_x + v_mid * slope_y + w_mid * slope_z
        return middle + FLOW_STEP * (-carried + VISCOSITY * laplace + forcing)
    next_u = advance(u_mid, u_dx, u_dy, u_dz, u_lap, drift_v * vort_z - load_x)
    next_v = advance(v_mid, v_dx, v_dy, v_dz, v_lap, -drift_u * vort_z - load_y)
    next_w = advance(w_mid, w_dx, w_dy, w_dz, w_lap, drift_u * vort_y - drift_v * vort_x)
    return jnp.stack([next_u, next_v, next_w])

def reference(surface_height, surface_potential, velocity):
    kx_values, kx_kept = wave_numbers(jnp.arange(NX, dtype=jnp.int32), NX)
    ky_values, ky_kept = wave_numbers(jnp.arange(NY, dtype=jnp.int32), NY)
    kx_grid = kx_values[None, :]
    ky_grid = ky_values[:, None]
    mask = ky_kept[:, None] * kx_kept[None, :]
    magnitude = jnp.sqrt(kx_grid * kx_grid + ky_grid * ky_grid)

    def forward(source):
        return jnp.fft.fft2(source) * mask

    def backward(spectrum, factor):
        return jnp.real(jnp.fft.ifft2(spectrum * factor))
    height = surface_height
    pot_hat = forward(surface_potential)
    height_hat = forward(height)
    vert_one = backward(pot_hat, magnitude)
    curve_one = backward(pot_hat, magnitude * magnitude)
    cube_one = backward(pot_hat, magnitude * magnitude * magnitude)
    pot_dx = backward(pot_hat, 1j * kx_grid)
    pot_dy = backward(pot_hat, 1j * ky_grid)
    height_dx = backward(height_hat, 1j * kx_grid)
    height_dy = backward(height_hat, 1j * ky_grid)
    second_pot = -height * vert_one
    second_hat = forward(second_pot)
    vert_two = backward(second_hat, magnitude)
    curve_two = backward(second_hat, magnitude * magnitude)
    third_pot = -height * vert_two - 0.5 * height * height * curve_one
    vert_three = backward(forward(third_pot), magnitude)
    vertical = vert_one + vert_two + vert_three + height * (curve_one + curve_two) + 0.5 * height * height * cube_one
    slope = height_dx * height_dx + height_dy * height_dy
    height_rate = -(height_dx * pot_dx + height_dy * pot_dy) + (1.0 + slope) * vertical
    potential_rate = -GRAVITY * height - 0.5 * (pot_dx * pot_dx + pot_dy * pot_dy) + 0.5 * (1.0 + slope) * vertical * vertical
    pressure = GRAVITY * coarsen(height + SURFACE_STEP * height_rate)
    surface_u = coarsen(pot_dx)
    surface_v = coarsen(pot_dy)
    padded_flow = jnp.pad(velocity, ((0, 0), (0, 0), (1, 1), (1, 1)), mode='wrap')
    padded_load = jnp.pad(pressure, ((1, 1), (1, 1)), mode='wrap')
    velocity_next = flow_update(padded_flow, padded_load, surface_u, surface_v)
    return (height_rate, potential_rate, velocity_next)
```

```python
import functools
import math

import jax
import jax.numpy as jnp
from jax import lax
from jax.experimental import pallas as pl
from jax.experimental.pallas import tpu as pltpu
from jax.sharding import PartitionSpec as P

COARSE = 2
GRAVITY = 1.0
SURFACE_STEP = 0.05
FLOW_STEP = 0.5
VISCOSITY = 0.2
DECAY_RATE = 0.05

F32 = jnp.float32
BF16 = jnp.bfloat16
VMEM_LIMIT = 60 * 1024 * 1024


def round_up(value, step):
    return -(-value // step) * step


class Plan:
    def __init__(self, rows, cols, tile):
        self.R, self.C = rows, cols
        self.NYL, self.NXL = tile
        self.NY, self.NX = rows * self.NYL, cols * self.NXL
        self.XC = self.NXL // rows
        self.Q = max(1, 128 // self.XC)
        self.NYF = self.NYL // self.Q
        self.W = self.Q * self.XC
        self.KEPT_Y = self.NY // 3 + 1
        self.KEPT_X = self.NX // 3 + 1
        self.M = round_up(-(-(-(-self.KEPT_Y // rows)) // cols), 8)
        self.KY = cols * self.M
        self.J = round_up(-(-self.KEPT_X // cols), 128)
        self.L2 = 2 * self.XC
        self.PEERS = rows * cols
        self.NYC, self.NXC = self.NYF // COARSE, self.W // COARSE


def split(x):
    hi = x.astype(BF16)
    return hi, (x - hi.astype(F32)).astype(BF16)


def dot(a, b):
    return jnp.dot(a, b, preferred_element_type=F32)


def dot3(a, b):
    return dot(a[0], b[0]) + (dot(a[0], b[1]) + dot(a[1], b[0]))


def cat(parts, axis):
    return parts[0] if len(parts) == 1 else jnp.concatenate(parts, axis=axis)


def turn(numer, denom):
    numer %= denom
    exact = {0: (1.0, 0.0), 1: (0.0, 1.0), 2: (-1.0, 0.0), 3: (0.0, -1.0)}
    if 4 * numer % denom == 0:
        return exact[4 * numer // denom]
    angle = 2.0 * math.pi * numer / denom
    return math.cos(angle), math.sin(angle)


def combine(terms):
    total = None
    for factor, value in terms:
        if factor == 0.0:
            continue
        if total is None:
            total = value if factor == 1.0 else (-value if factor == -1.0 else factor * value)
        elif factor == 1.0:
            total = total + value
        elif factor == -1.0:
            total = total - value
        else:
            total = total + factor * value
    return total


def mirrored(index, count):
    if index == 0 or 2 * index == count:
        return ((index, 1.0),)
    return ((index, 1.0), (count - index, -1.0))


def unfold(x, plan):
    return cat([x[:, h * plan.XC : (h + 1) * plan.XC] for h in range(plan.Q)], 0)


def fold(x, plan):
    return cat([x[h * plan.NYF : (h + 1) * plan.NYF] for h in range(plan.Q)], 1)


def swap_halves(x, half):
    if 2 * half == 128:
        return pltpu.roll(x, half, 1)
    return jnp.concatenate([x[:, half:], x[:, :half]], axis=1)


def y_forward(plan, blocks, field, tab, out_ref):
    for k0 in range(plan.R // 2 + 1):
        even = combine([(turn(k0 * r, plan.R)[0], blocks[r]) for r in range(plan.R)])
        odd = combine([(turn(k0 * r, plan.R)[1], blocks[r]) for r in range(plan.R)])
        even = split(unfold(even, plan))
        if odd is None:
            odd = tuple(jnp.zeros_like(e) for e in even)
        else:
            odd = split(unfold(odd, plan))
        for k, sign in mirrored(k0, plan.R):
            if sign > 0:
                pos, neg = odd, [-o for o in odd]
            else:
                pos, neg = [-o for o in odd], odd
            rhs = [
                jnp.concatenate(
                    [
                        jnp.concatenate([even[i], pos[i]], axis=1),
                        jnp.concatenate([neg[i], even[i]], axis=1),
                    ],
                    axis=0,
                )
                for i in range(2)
            ]
            lines = dot3((tab[0][k], tab[1][k]), rhs)
            for c in range(plan.C):
                out_ref[k * plan.C + c, field * plan.M : (field + 1) * plan.M, :] = lines[
                    c * plan.M : (c + 1) * plan.M
                ]


def y_inverse(plan, buf_ref, fields, tab, work_ref):
    L2, M, C = plan.L2, plan.M, plan.C
    lane = lax.broadcasted_iota(jnp.int32, (1, L2), 1)
    flip = jnp.where(lane < plan.XC, 1.0, -1.0).astype(F32)
    for k0 in range(plan.R // 2 + 1):
        total = None
        for k, sign in mirrored(k0, plan.R):
            tops, bottoms = [], []
            for f in range(fields):
                lines = cat(
                    [buf_ref[k * C + c, f * M : (f + 1) * M, :] for c in range(C)], 0
                )
                tops.append(lines)
                bottoms.append(swap_halves(lines, plan.XC) * flip)
            rhs = split(jnp.concatenate([cat(tops, 1), cat(bottoms, 1)], axis=0))
            part = dot3((tab[0][k], tab[1][k]), rhs)
            if sign > 0:
                total = part
            else:
                total = total + part * cat([flip] * fields, 1)
        work_ref[k0] = total


def y_block(plan, work_ref, field, r):
    L2 = plan.L2
    lane = lax.broadcasted_iota(jnp.int32, (1, L2), 1)
    total = None
    for k0 in range(plan.R // 2 + 1):
        c, s = turn(k0 * r, plan.R)
        factor = jnp.where(lane < plan.XC, c, s).astype(F32)
        part = work_ref[k0, :, field * L2 : (field + 1) * L2] * factor
        total = part if total is None else total + part
    if L2 == 128 and plan.Q == 2:
        both = total + pltpu.roll(total, plan.XC, 1)
        return jnp.where(lane < plan.XC, both[: plan.NYF], both[plan.NYF :])
    return fold(total[:, : plan.XC] + total[:, plan.XC :], plan)


def pack_kernel(plan, potential_ref, height_ref, out_ref):
    for r in range(plan.R):
        for f, ref in enumerate((potential_ref, height_ref)):
            out_ref[r, f * plan.NYF : (f + 1) * plan.NYF, :] = fold(
                ref[:, r * plan.XC : (r + 1) * plan.XC], plan
            )


def first_kernel(plan, in_ref, hi_ref, lo_ref, out_ref, height_ref):
    for f in range(2):
        blocks = [in_ref[r, f * plan.NYF : (f + 1) * plan.NYF, :] for r in range(plan.R)]
        y_forward(plan, blocks, f, (hi_ref, lo_ref), out_ref)
    for r in range(plan.R):
        height_ref[r] = in_ref[r, plan.NYF :, :]


def x_kernel(plan, fields, wanted, place_ref, in_ref, fh, fl, ih, il, out_ref, u_ref):
    R, C, M, J, XC, NXL = plan.R, plan.C, plan.M, plan.J, plan.XC, plan.NXL
    rows, outs = fields * M, len(wanted)
    lines = []
    for c in range(C):
        halves = []
        for h in range(2):
            halves.append(
                cat([in_ref[r * C + c, :, h * XC : (h + 1) * XC] for r in range(R)], 1)
            )
        lines.append(jnp.concatenate(halves, axis=0))
    row_k0, row_k1 = place_ref[0], place_ref[1]
    ky_index = R * (row_k1 + lax.broadcasted_iota(jnp.int32, (M, J), 0)) + row_k0
    ky = ky_index.astype(F32) * (2.0 * math.pi / plan.NY)
    y_weight = jnp.where(
        ky_index == 0, 1.0, jnp.where(ky_index < plan.KEPT_Y, 2.0, 0.0)
    ).astype(F32)
    slot = 0
    slots = []
    for j0 in range(C // 2 + 1):
        even = split(combine([(turn(j0 * c, C)[0], lines[c]) for c in range(C)]))
        odd = combine([(turn(j0 * c, C)[1], lines[c]) for c in range(C)])
        odd = None if odd is None else split(odd)
        u_sum = v_sum = None
        for j, sign in mirrored(j0, C):
            table = (fh[j], fl[j])
            of_even = dot3(even, table)
            p_all, q_all = of_even[:, :J], of_even[:, J:]
            if odd is not None:
                of_odd = dot3(odd, table)
                p_all = p_all - sign * of_odd[:, J:]
                q_all = q_all + sign * of_odd[:, :J]
            kx_index = C * lax.broadcasted_iota(jnp.int32, (M, J), 1) + j
            kx = kx_index.astype(F32) * (2.0 * math.pi / plan.NX)
            x_weight = jnp.where(
                kx_index == 0, 1.0, jnp.where(kx_index < plan.KEPT_X, 2.0, 0.0)
            ).astype(F32)
            weight = x_weight * y_weight * (1.0 / (plan.NX * plan.NY))
            size = jnp.sqrt(kx * kx + ky * ky)
            coef = []
            for f in range(fields):
                top, low = slice(f * M, (f + 1) * M), slice(rows + f * M, rows + (f + 1) * M)
                coef.append(
                    (
                        p_all[top] * weight,
                        q_all[top] * weight,
                        p_all[low] * weight,
                        q_all[low] * weight,
                    )
                )
            tops, lows = [], []
            for f, kind in wanted:
                cc, cs, sc, ss = coef[f]
                if kind == "dx":
                    new = (kx * cs, -kx * cc, kx * ss, -kx * sc)
                elif kind == "dy":
                    new = (ky * sc, ky * ss, -ky * cc, -ky * cs)
                else:
                    factor = size
                    for _ in range(kind - 1):
                        factor = factor * size
                    new = (factor * cc, factor * cs, factor * sc, factor * ss)
                tops.append((new[0], new[1]))
                lows.append((new[2], new[3]))
            p_new = cat([t[0] for t in tops] + [t[0] for t in lows], 0)
            q_new = cat([t[1] for t in tops] + [t[1] for t in lows], 0)
            p_new, q_new = split(p_new), split(q_new)
            back = (ih[j], il[j])
            u = dot3([jnp.concatenate([p_new[i], q_new[i]], axis=1) for i in range(2)], back)
            u_sum = u if u_sum is None else u_sum + u
            if odd is not None:
                v = dot3(
                    [jnp.concatenate([q_new[i], -p_new[i]], axis=1) for i in range(2)], back
                )
                v_sum = v if v_sum is None else v_sum - v
        u_ref[slot] = u_sum
        slots.append((j0, slot, None if v_sum is None else slot + 1))
        if v_sum is not None:
            u_ref[slot + 1] = v_sum
        slot += 1 if v_sum is None else 2
    half = outs * M
    for c in range(C):
        terms = []
        for j0, u_slot, v_slot in slots:
            cs, sn = turn(j0 * c, C)
            terms.append((cs, u_slot))
            if v_slot is not None:
                terms.append((sn, v_slot))
        for r in range(0, R):
            lanes = slice(r * XC, (r + 1) * XC)
            top = combine([(a, u_ref[s, :half, lanes]) for a, s in terms if a != 0.0])
            low = combine([(a, u_ref[s, half:, lanes]) for a, s in terms if a != 0.0])
            out_ref[r * C + c] = jnp.concatenate([top, low], axis=1)


def second_kernel(
    plan, buf_ref, height_ref, ih, il, fh, fl,
    out_ref, vertical_ref, third_ref, slope_ref, rate_ref, energy_ref, coarse_ref, work_ref,
):
    y_inverse(plan, buf_ref, 7, (ih, il), work_ref)
    pool_y, pool_x = pools(plan.NYC, plan.NYF, plan.W, plan.NXC)
    blocks = []
    for r in range(plan.R):
        height = height_ref[r]
        vert, curve, cube, pot_dx, pot_dy, height_dx, height_dy = [
            y_block(plan, work_ref, f, r) for f in range(7)
        ]
        square = 0.5 * height * height
        vertical_ref[r] = vert + height * curve + square * cube
        third_ref[r] = -square * curve
        slope_ref[r] = height_dx * height_dx + height_dy * height_dy
        rate_ref[r] = -(height_dx * pot_dx + height_dy * pot_dy)
        energy_ref[r] = -GRAVITY * height - 0.5 * (pot_dx * pot_dx + pot_dy * pot_dy)
        coarse_ref[r] = jnp.concatenate(
            [pooled(pot_dx, pool_y, pool_x), pooled(pot_dy, pool_y, pool_x)], axis=1
        )
        blocks.append(-height * vert)
    y_forward(plan, blocks, 0, (fh, fl), out_ref)


def third_kernel(
    plan, buf_ref, height_ref, vertical_in, third_in, ih, il, fh, fl, out_ref, vertical_ref, work_ref
):
    y_inverse(plan, buf_ref, 2, (ih, il), work_ref)
    blocks = []
    for r in range(plan.R):
        height = height_ref[r]
        vert, curve = [y_block(plan, work_ref, f, r) for f in range(2)]
        vertical_ref[r] = vertical_in[r] + vert + height * curve
        blocks.append(third_in[r] - height * vert)
    y_forward(plan, blocks, 0, (fh, fl), out_ref)


def rates_kernel(
    plan, buf_ref, vertical_in, slope_ref, rate_ref, energy_ref, coarse_ref, ih, il, out_ref, work_ref
):
    y_inverse(plan, buf_ref, 1, (ih, il), work_ref)
    N = plan.NYF
    for r in range(plan.R):
        vertical = vertical_in[r] + y_block(plan, work_ref, 0, r)
        lift = (1.0 + slope_ref[r]) * vertical
        out_ref[r, :N, :] = rate_ref[r] + lift
        out_ref[r, N : 2 * N, :] = energy_ref[r] + 0.5 * lift * vertical
        out_ref[r, 2 * N :, :] = coarse_ref[r]


def pools(rows_out, rows_in, cols_in, cols_out):
    def pool(shape, out_dim):
        i = lax.broadcasted_iota(jnp.int32, shape, out_dim)
        k = lax.broadcasted_iota(jnp.int32, shape, 1 - out_dim)
        return jnp.where((k >= COARSE * i) & (k < COARSE * (i + 1)), 1.0 / COARSE, 0.0).astype(BF16)

    return pool((rows_out, rows_in), 0), pool((cols_in, cols_out), 1)


def pooled(x, pool_y, pool_x):
    hi, lo = split(x)
    low = (x - hi.astype(F32) - lo.astype(F32)).astype(BF16)
    lines = dot(hi, pool_x) + (dot(lo, pool_x) + dot(low, pool_x))
    hi, lo = split(lines)
    low = (lines - hi.astype(F32) - lo.astype(F32)).astype(BF16)
    return dot(pool_y, hi) + (dot(pool_y, lo) + dot(pool_y, low))


def tile_kernel(
    plan, in_ref, height_ref, rate_ref, energy_ref, pressure_ref, u_ref, v_ref, column_ref
):
    R, Q, XC, N = plan.R, plan.Q, plan.XC, plan.NYF
    for f, ref in enumerate((rate_ref, energy_ref)):
        for h in range(Q):
            ref[h * N : (h + 1) * N, :] = cat(
                [in_ref[r, f * N : (f + 1) * N, h * XC : (h + 1) * XC] for r in range(R)], 1
            )
    NC, XH = plan.NYC, XC // COARSE
    for f, ref in enumerate((u_ref, v_ref)):
        for h in range(Q):
            base = f * plan.NXC + h * XH
            ref[h * NC : (h + 1) * NC, :] = cat(
                [in_ref[r, 2 * N :, base : base + XH] for r in range(R)], 1
            )
    pool_y, pool_x = pools(plan.NYL // COARSE, plan.NYL, plan.NXL, plan.NXL // COARSE)
    pressure = GRAVITY * pooled(height_ref[...] + SURFACE_STEP * rate_ref[...], pool_y, pool_x)
    pressure_ref[...] = pressure
    first = jnp.transpose(pressure[:, :128])
    last = jnp.transpose(pressure[:, -128:])
    column_ref[0:8, :] = first[0:8]
    column_ref[8:16, :] = last[-8:]


def flow_kernel(
    levels, decay_ref, prev_ref, cur_ref, next_ref, rows_ref, cols_ref,
    pressure_ref, prow_ref, pcol_ref, u_ref, v_ref, out_ref,
):
    level = pl.program_id(0)
    ny, nx = cur_ref.shape[2:]
    lane = lax.broadcasted_iota(jnp.int32, (ny, nx), 1)
    line = lax.broadcasted_iota(jnp.int32, (ny, nx), 0)

    def around(x, south, north, west, east):
        return (
            jnp.where(lane == nx - 1, east, pltpu.roll(x, nx - 1, 1)),
            jnp.where(lane == 0, west, pltpu.roll(x, 1, 1)),
            jnp.where(line == ny - 1, north, pltpu.roll(x, ny - 1, 0)),
            jnp.where(line == 0, south, pltpu.roll(x, 1, 0)),
        )

    cols = jnp.transpose(cols_ref[0])
    top_u, top_v = u_ref[...], v_ref[...]
    is_top = level == 0

    def derivs(q, top):
        mid = cur_ref[q, 0]
        east, west, north, south = around(
            mid,
            rows_ref[0, q : q + 1, :],
            rows_ref[0, 3 + q : 4 + q, :],
            cols[:, q : q + 1],
            cols[:, 3 + q : 4 + q],
        )
        above = jnp.where(is_top, top, prev_ref[q, 0])
        below = next_ref[q, 0]
        lap = (east + west) + (north + south) + (above + below) - 6.0 * mid
        return mid, 0.5 * (east - west), 0.5 * (north - south), 0.5 * (above - below), lap

    u, u_dx, u_dy, u_dz, u_lap = derivs(0, top_u)
    v, v_dx, v_dy, v_dz, v_lap = derivs(1, top_v)
    w, w_dx, w_dy, w_dz, w_lap = derivs(2, jnp.zeros_like(top_u))
    drift_u = top_u * decay_ref[level, 0]
    drift_v = top_v * decay_ref[level, 0]
    vort_x = w_dy - v_dz
    vort_y = u_dz - w_dx
    vort_z = v_dx - u_dy
    pcols = jnp.transpose(pcol_ref[...])
    p_east, p_west, p_north, p_south = around(
        pressure_ref[...], prow_ref[0:1, :], prow_ref[1:2, :], pcols[:, 0:1], pcols[:, 1:2]
    )
    load = 0.5 * decay_ref[level, 1]
    load_x = load * (p_east - p_west)
    load_y = load * (p_north - p_south)

    def advance(mid, dx, dy, dz, lap, force):
        return mid + FLOW_STEP * (VISCOSITY * lap + force - (u * dx + v * dy + w * dz))

    out_ref[0, 0] = advance(u, u_dx, u_dy, u_dz, u_lap, drift_v * vort_z - load_x)
    out_ref[1, 0] = advance(v, v_dx, v_dy, v_dz, v_lap, -drift_u * vort_z - load_y)
    out_ref[2, 0] = advance(w, w_dx, w_dy, w_dz, w_lap, drift_u * vort_y - drift_v * vort_x)


def parts(table):
    hi = lax.reduce_precision(table, 8, 7)
    return hi.astype(BF16), (table - hi).astype(BF16)


def angles(numbers, places, total):
    numbers, places = lax.optimization_barrier((numbers, places))
    return (numbers * places % total).astype(F32) * (2.0 * math.pi / total)


def make_tables(plan):
    k0 = jnp.arange(plan.R, dtype=jnp.int32)[:, None, None]
    k1 = jnp.arange(plan.KY, dtype=jnp.int32)
    y = jnp.arange(plan.NYL, dtype=jnp.int32)
    angle = angles(plan.R * k1[None, :, None] + k0, y[None, None, :], plan.NY)
    y_fwd = parts(jnp.concatenate([jnp.cos(angle), jnp.sin(angle)], axis=2))
    angle = angles(plan.R * k1[None, None, :] + k0, y[None, :, None], plan.NY)
    y_inv = parts(jnp.concatenate([jnp.cos(angle), jnp.sin(angle)], axis=2))
    j0 = jnp.arange(plan.C, dtype=jnp.int32)[:, None, None]
    j1 = jnp.arange(plan.J, dtype=jnp.int32)
    x = jnp.arange(plan.NXL, dtype=jnp.int32)
    angle = angles(plan.C * j1[None, None, :] + j0, x[None, :, None], plan.NX)
    x_fwd = parts(jnp.concatenate([jnp.cos(angle), jnp.sin(angle)], axis=2))
    angle = angles(plan.C * j1[None, :, None] + j0, x[None, None, :], plan.NX)
    x_inv = parts(jnp.concatenate([jnp.cos(angle), jnp.sin(angle)], axis=1))
    return y_fwd, y_inv, x_fwd, x_inv


def call(kernel, name, outs, scratch=(), smem=0):
    vmem = pl.BlockSpec(memory_space=pltpu.VMEM)

    def run(*args):
        specs = [pl.BlockSpec(memory_space=pltpu.SMEM)] * smem + [vmem] * (len(args) - smem)
        shapes = [jax.ShapeDtypeStruct(s, F32) for s in outs]
        return pl.pallas_call(
            kernel,
            out_shape=shapes,
            in_specs=specs,
            out_specs=[vmem] * len(outs),
            scratch_shapes=[pltpu.VMEM(s, F32) for s in scratch],
            compiler_params=pltpu.CompilerParams(vmem_limit_bytes=VMEM_LIMIT),
            name=name,
        )(*args)

    return run


def exchange(x, axes):
    return lax.all_to_all(x, axes, split_axis=0, concat_axis=0, tiled=True)


def shift(x, axis, step):
    peers = lax.axis_size(axis)
    return lax.ppermute(x, axis, [(i, (i + step) % peers) for i in range(peers)])


def local(surface_height, surface_potential, velocity):
    plan = Plan(lax.axis_size("row"), lax.axis_size("col"), surface_height.shape)
    R, M, W, N, L2 = plan.R, plan.M, plan.W, plan.NYF, plan.L2
    bind = lambda kernel, *rest: functools.partial(kernel, plan, *rest)
    both = ("row", "col")
    pencil = (R, N, W)
    work = lambda f: (R // 2 + 1, plan.NYL, f * L2)
    spec = lambda f: (plan.PEERS, f * M, L2)

    (packed,) = call(bind(pack_kernel), "pack", [(R, 2 * N, W)])(surface_potential, surface_height)
    packed = exchange(packed, "row")

    levels, ny, nx = velocity.shape[1:]
    rows = jnp.concatenate(
        [shift(velocity[:, :, -1, :], "row", 1), shift(velocity[:, :, 0, :], "row", -1)], axis=0
    )
    cols = jnp.concatenate(
        [shift(velocity[:, :, :, -1], "col", 1), shift(velocity[:, :, :, 0], "col", -1)], axis=0
    )
    pad = lambda e: jnp.pad(jnp.swapaxes(e, 0, 1), ((0, 0), (0, 2), (0, 0)))
    rows, cols = pad(rows), pad(cols)
    mid = jnp.arange(levels, dtype=F32) + 0.5
    decay = jnp.stack([jnp.exp(-2.0 * DECAY_RATE * mid), jnp.exp(-DECAY_RATE * mid)], axis=1)

    y_fwd, y_inv, x_fwd, x_inv = make_tables(plan)
    place = jnp.stack([lax.axis_index("row"), lax.axis_index("col") * M]).astype(jnp.int32)

    def x_stage(buf, fields, wanted):
        outs = len(wanted)
        slots = 2 * (plan.C // 2 + 1) - (1 if plan.C == 1 else 2)
        kernel = bind(x_kernel, fields, wanted)
        (out,) = call(
            kernel, "x%d" % outs, [spec(outs)], [(slots, 2 * outs * M, plan.NXL)], smem=1
        )(place, buf, *x_fwd, *x_inv)
        return exchange(out, both)

    first, height = call(bind(first_kernel), "y0", [spec(2), pencil])(packed, *y_fwd)
    first = x_stage(
        exchange(first, both),
        2,
        ((0, 1), (0, 2), (0, 3), (0, "dx"), (0, "dy"), (1, "dx"), (1, "dy")),
    )
    second, vertical, third, slope, rate, energy, coarse = call(
        bind(second_kernel),
        "y1",
        [spec(1)] + [pencil] * 5 + [(R, plan.NYC, 2 * plan.NXC)],
        [work(7)],
    )(first, height, *y_inv, *y_fwd)
    second = x_stage(exchange(second, both), 1, ((0, 1), (0, 2)))
    last, vertical = call(bind(third_kernel), "y2", [spec(1), pencil], [work(2)])(
        second, height, vertical, third, *y_inv, *y_fwd
    )
    last = x_stage(exchange(last, both), 1, ((0, 1),))
    (rates,) = call(bind(rates_kernel), "y3", [(R, 2 * N + plan.NYC, W)], [work(1)])(
        last, vertical, slope, rate, energy, coarse, *y_inv
    )
    rates = exchange(rates, "row")
    tile = surface_height.shape
    height_rate, potential_rate, pressure, surface_u, surface_v, column = call(
        bind(tile_kernel), "tile", [tile, tile] + [(ny, nx)] * 3 + [(16, ny)]
    )(rates, surface_height)

    prow = jnp.concatenate(
        [shift(pressure[-1:], "row", 1), shift(pressure[:1], "row", -1)], axis=0
    )
    pcol = jnp.concatenate(
        [shift(column[-1:], "col", 1), shift(column[:1], "col", -1)], axis=0
    )
    prow, pcol = [jnp.pad(e, ((0, 6), (0, 0))) for e in (prow, pcol)]

    block = (3, 1, ny, nx)
    at = lambda step: pl.BlockSpec(
        block, lambda l: (0, jnp.clip(l + step, 0, levels - 1), 0, 0)
    )
    whole = lambda x: pl.BlockSpec(x.shape, lambda l: (0,) * x.ndim)
    per_level = lambda x: pl.BlockSpec((1,) + x.shape[1:], lambda l: (l, 0, 0))
    velocity_next = pl.pallas_call(
        functools.partial(flow_kernel, levels),
        grid=(levels,),
        out_shape=jax.ShapeDtypeStruct(velocity.shape, F32),
        in_specs=[pl.BlockSpec(memory_space=pltpu.SMEM), at(-1), at(0), at(1)]
        + [per_level(rows), per_level(cols)]
        + [whole(x) for x in (pressure, prow, pcol, surface_u, surface_v)],
        out_specs=at(0),
        compiler_params=pltpu.CompilerParams(vmem_limit_bytes=VMEM_LIMIT),
        name="flow",
    )(decay, velocity, velocity, velocity, rows, cols, pressure, prow, pcol, surface_u, surface_v)
    return height_rate, potential_rate, velocity_next


def solution(mesh):
    placed = (P("row", "col"), P("row", "col"), P(None, None, "row", "col"))
    return jax.shard_map(
        local,
        mesh=mesh,
        in_specs=placed,
        out_specs=placed,
        check_vma=False,
    )
```

```python
import functools
import math

import jax
import jax.numpy as jnp
from jax import lax
from jax.experimental import pallas as pl
from jax.experimental.pallas import tpu as pltpu
from jax.sharding import PartitionSpec as P

COARSE = 2
GRAVITY = 1.0
SURFACE_STEP = 0.05
FLOW_STEP = 0.5
VISCOSITY = 0.2
DECAY_RATE = 0.05

F32 = jnp.float32
BF16 = jnp.bfloat16
MIB = 1024 * 1024


def round_up(value, step):
    return -(-value // step) * step


class Plan:
    def __init__(self, rows, cols, tile):
        self.R, self.C = rows, cols
        self.NYL, self.NXL = tile
        self.NY, self.NX = rows * self.NYL, cols * self.NXL
        self.XC = self.NXL // rows
        self.Q = max(1, 128 // self.XC)
        self.NYF = self.NYL // self.Q
        self.W = self.Q * self.XC
        self.KEPT_Y = self.NY // 3 + 1
        self.KEPT_X = self.NX // 3 + 1
        self.M = round_up(-(-(-(-self.KEPT_Y // rows)) // cols), 8)
        self.KY = cols * self.M
        self.J = round_up(-(-self.KEPT_X // cols), 128)
        self.L2 = 2 * self.XC
        self.PEERS = rows * cols
        self.NYC, self.NXC = self.NYF // COARSE, self.W // COARSE


def split(x):
    hi = x.astype(BF16)
    return hi, (x - hi.astype(F32)).astype(BF16)


def dot(a, b, flipped=False):
    dims = (((1,), (1 if flipped else 0,)), ((), ()))
    return lax.dot_general(a, b, dims, preferred_element_type=F32)


def cat(parts, axis):
    return parts[0] if len(parts) == 1 else jnp.concatenate(parts, axis=axis)


def turn(numer, denom):
    numer %= denom
    exact = {0: (1.0, 0.0), 1: (0.0, 1.0), 2: (-1.0, 0.0), 3: (0.0, -1.0)}
    if 4 * numer % denom == 0:
        return exact[4 * numer // denom]
    angle = 2.0 * math.pi * numer / denom
    return math.cos(angle), math.sin(angle)


def combine(terms):
    total = None
    for factor, value in terms:
        if factor == 0.0:
            continue
        if total is None:
            total = value if factor == 1.0 else (-value if factor == -1.0 else factor * value)
        elif factor == 1.0:
            total = total + value
        elif factor == -1.0:
            total = total - value
        else:
            total = total + factor * value
    return total


def mirrored(index, count):
    if index == 0 or 2 * index == count:
        return ((index, 1.0),)
    return ((index, 1.0), (count - index, -1.0))


def unfold(x, plan):
    return cat([x[:, h * plan.XC : (h + 1) * plan.XC] for h in range(plan.Q)], 0)


def fold(x, plan):
    return cat([x[h * plan.NYF : (h + 1) * plan.NYF] for h in range(plan.Q)], 1)


def swap_halves(x, half):
    if 2 * half == 128:
        return pltpu.roll(x, half, 1)
    return jnp.concatenate([x[:, half:], x[:, :half]], axis=1)


def table_rows(table, rhs):
    rows = table.shape[0] // 2
    both = dot(table, rhs[0])
    return both[:rows] + (both[rows:] + dot(table[:rows], rhs[1]))


def y_forward(plan, blocks, field, tab, out_ref):
    for k0 in range(plan.R // 2 + 1):
        even = combine([(turn(k0 * r, plan.R)[0], blocks[r]) for r in range(plan.R)])
        odd = combine([(turn(k0 * r, plan.R)[1], blocks[r]) for r in range(plan.R)])
        even = split(unfold(even, plan))
        if odd is None:
            odd = tuple(jnp.zeros_like(e) for e in even)
        else:
            odd = split(unfold(odd, plan))
        for k, sign in mirrored(k0, plan.R):
            if sign > 0:
                pos, neg = odd, [-o for o in odd]
            else:
                pos, neg = [-o for o in odd], odd
            rhs = [
                jnp.concatenate(
                    [
                        jnp.concatenate([even[i], pos[i]], axis=1),
                        jnp.concatenate([neg[i], even[i]], axis=1),
                    ],
                    axis=0,
                )
                for i in range(2)
            ]
            lines = table_rows(tab[k], rhs)
            for c in range(plan.C):
                out_ref[k * plan.C + c, field * plan.M : (field + 1) * plan.M, :] = lines[
                    c * plan.M : (c + 1) * plan.M
                ]


def y_inverse(plan, buf_ref, fields, tab, work_ref):
    L2, M, C = plan.L2, plan.M, plan.C
    lane = lax.broadcasted_iota(jnp.int32, (1, L2), 1)
    flip = jnp.where(lane < plan.XC, 1.0, -1.0).astype(F32)
    for k0 in range(plan.R // 2 + 1):
        total = None
        for k, sign in mirrored(k0, plan.R):
            tops, bottoms = [], []
            for f in range(fields):
                lines = cat(
                    [buf_ref[k * C + c, f * M : (f + 1) * M, :] for c in range(C)], 0
                )
                tops.append(lines)
                bottoms.append(swap_halves(lines, plan.XC) * flip)
            rhs = split(jnp.concatenate([cat(tops, 1), cat(bottoms, 1)], axis=0))
            part = table_rows(tab[k], rhs)
            if sign > 0:
                total = part
            else:
                total = total + part * cat([flip] * fields, 1)
        work_ref[k0] = total


def y_block(plan, work_ref, field, r):
    L2 = plan.L2
    lane = lax.broadcasted_iota(jnp.int32, (1, L2), 1)
    total = None
    for k0 in range(plan.R // 2 + 1):
        c, s = turn(k0 * r, plan.R)
        factor = jnp.where(lane < plan.XC, c, s).astype(F32)
        part = work_ref[k0, :, field * L2 : (field + 1) * L2] * factor
        total = part if total is None else total + part
    if L2 == 128 and plan.Q == 2:
        both = total + pltpu.roll(total, plan.XC, 1)
        return jnp.where(lane < plan.XC, both[: plan.NYF], both[plan.NYF :])
    return fold(total[:, : plan.XC] + total[:, plan.XC :], plan)


def pack_kernel(plan, potential_ref, height_ref, out_ref):
    for r in range(plan.R):
        for f, ref in enumerate((potential_ref, height_ref)):
            out_ref[r, f * plan.NYF : (f + 1) * plan.NYF, :] = fold(
                ref[:, r * plan.XC : (r + 1) * plan.XC], plan
            )


def first_kernel(plan, in_ref, yf, out_ref, height_ref):
    for f in range(2):
        blocks = [in_ref[r, f * plan.NYF : (f + 1) * plan.NYF, :] for r in range(plan.R)]
        y_forward(plan, blocks, f, yf, out_ref)
    for r in range(plan.R):
        height_ref[r] = in_ref[r, plan.NYF :, :]


def stacked(pair, table_hi, table_lo, flipped=False):
    hi = cat([p[0] for p in pair], 0)
    lo = cat([p[1] for p in pair], 0)
    rows = hi.shape[0]
    both = dot(jnp.concatenate([hi, lo], axis=0), table_hi, flipped)
    total = both[:rows] + (both[rows:] + dot(hi, table_lo, flipped))
    rows = pair[0][0].shape[0]
    return [total[i * rows : (i + 1) * rows] for i in range(len(pair))]


def x_kernel(
    plan, sources, wanted, place_ref, in_ref, fh, fl, out_ref, u_ref,
):
    R, C, M, J, XC, NXL = plan.R, plan.C, plan.M, plan.J, plan.XC, plan.NXL
    fields, outs = len(sources), len(wanted)
    rows = fields * M
    lines = []
    for c in range(C):
        parts_of = []
        for h in range(2):
            for f in sources:
                parts_of.append(
                    cat(
                        [
                            in_ref[r * C + c, f * M : (f + 1) * M, h * XC : (h + 1) * XC]
                            for r in range(R)
                        ],
                        1,
                    )
                )
        lines.append(jnp.concatenate(parts_of, axis=0))
    row_k0, row_k1 = place_ref[0], place_ref[1]
    ky_index = R * (row_k1 + lax.broadcasted_iota(jnp.int32, (M, J), 0)) + row_k0
    ky = ky_index.astype(F32) * (2.0 * math.pi / plan.NY)
    y_weight = jnp.where(
        ky_index == 0, 1.0, jnp.where(ky_index < plan.KEPT_Y, 2.0, 0.0)
    ).astype(F32)
    slot = 0
    slots = []
    for j0 in range(C // 2 + 1):
        pair = [split(combine([(turn(j0 * c, C)[0], lines[c]) for c in range(C)]))]
        odd = combine([(turn(j0 * c, C)[1], lines[c]) for c in range(C)])
        if odd is not None:
            pair.append(split(odd))
        u_sum = v_sum = None
        for j, sign in mirrored(j0, C):
            found = stacked(pair, fh[j], fl[j])
            p_all, q_all = found[0][:, :J], found[0][:, J:]
            if odd is not None:
                p_all = p_all - sign * found[1][:, J:]
                q_all = q_all + sign * found[1][:, :J]
            kx_index = C * lax.broadcasted_iota(jnp.int32, (M, J), 1) + j
            kx = kx_index.astype(F32) * (2.0 * math.pi / plan.NX)
            x_weight = jnp.where(
                kx_index == 0, 1.0, jnp.where(kx_index < plan.KEPT_X, 2.0, 0.0)
            ).astype(F32)
            weight = x_weight * y_weight * (1.0 / (plan.NX * plan.NY))
            size = jnp.sqrt(kx * kx + ky * ky)
            coef = []
            for f in range(fields):
                top, low = slice(f * M, (f + 1) * M), slice(rows + f * M, rows + (f + 1) * M)
                coef.append(
                    (
                        p_all[top] * weight,
                        q_all[top] * weight,
                        p_all[low] * weight,
                        q_all[low] * weight,
                    )
                )
            tops, lows = [], []
            for f, kind in wanted:
                cc, cs, sc, ss = coef[f]
                if kind == "dx":
                    new = (kx * cs, -kx * cc, kx * ss, -kx * sc)
                elif kind == "dy":
                    new = (ky * sc, ky * ss, -ky * cc, -ky * cs)
                else:
                    factor = size
                    for _ in range(kind - 1):
                        factor = factor * size
                    new = (factor * cc, factor * cs, factor * sc, factor * ss)
                tops.append((new[0], new[1]))
                lows.append((new[2], new[3]))
            p_new = split(cat([t[0] for t in tops] + [t[0] for t in lows], 0))
            q_new = split(cat([t[1] for t in tops] + [t[1] for t in lows], 0))
            pair_back = [[jnp.concatenate([p_new[i], q_new[i]], axis=1) for i in range(2)]]
            if odd is not None:
                pair_back.append(
                    [jnp.concatenate([q_new[i], -p_new[i]], axis=1) for i in range(2)]
                )
            found = stacked(pair_back, fh[j], fl[j], True)
            u_sum = found[0] if u_sum is None else u_sum + found[0]
            if odd is not None:
                v_sum = found[1] if v_sum is None else v_sum - found[1]
        u_ref[slot] = u_sum
        slots.append((j0, slot, None if v_sum is None else slot + 1))
        if v_sum is not None:
            u_ref[slot + 1] = v_sum
        slot += 1 if v_sum is None else 2
    half = outs * M
    for c in range(C):
        terms = []
        for j0, u_slot, v_slot in slots:
            cs, sn = turn(j0 * c, C)
            terms.append((cs, u_slot))
            if v_slot is not None:
                terms.append((sn, v_slot))
        for r in range(0, R):
            lanes = slice(r * XC, (r + 1) * XC)
            top = combine([(a, u_ref[s, :half, lanes]) for a, s in terms if a != 0.0])
            low = combine([(a, u_ref[s, half:, lanes]) for a, s in terms if a != 0.0])
            out_ref[r * C + c] = jnp.concatenate([top, low], axis=1)


def second_kernel(
    plan, buf_ref, height_ref, yi, yf, out_ref, vert_ref, work_ref
):
    y_inverse(plan, buf_ref, 1, yi, work_ref)
    blocks = []
    for r in range(plan.R):
        vert = y_block(plan, work_ref, 0, r)
        vert_ref[r] = vert
        blocks.append(-height_ref[r] * vert)
    y_forward(plan, blocks, 0, yf, out_ref)


def fields_kernel(
    plan, buf_ref, height_ref, vert_ref, yi,
    vertical_ref, third_ref, slope_ref, rate_ref, energy_ref, coarse_ref,
    work_ref,
):
    y_inverse(plan, buf_ref, 6, yi, work_ref)
    pool_y, pool_x = pools(plan.NYC, plan.NYF, plan.W, plan.NXC)
    for r in range(plan.R):
        height = height_ref[r]
        curve, cube, pot_dx, pot_dy, height_dx, height_dy = [
            y_block(plan, work_ref, f, r) for f in range(6)
        ]
        square = 0.5 * height * height
        vertical_ref[r] = vert_ref[r] + height * curve + square * cube
        third_ref[r] = -square * curve
        slope_ref[r] = height_dx * height_dx + height_dy * height_dy
        rate_ref[r] = -(height_dx * pot_dx + height_dy * pot_dy)
        energy_ref[r] = -GRAVITY * height - 0.5 * (pot_dx * pot_dx + pot_dy * pot_dy)
        coarse_ref[r] = jnp.concatenate(
            [pooled(pot_dx, pool_y, pool_x), pooled(pot_dy, pool_y, pool_x)], axis=1
        )


def third_kernel(
    plan, buf_ref, height_ref, vertical_in, third_in, yi, yf, out_ref, vertical_ref,
    work_ref,
):
    y_inverse(plan, buf_ref, 2, yi, work_ref)
    blocks = []
    for r in range(plan.R):
        height = height_ref[r]
        vert, curve = [y_block(plan, work_ref, f, r) for f in range(2)]
        vertical_ref[r] = vertical_in[r] + vert + height * curve
        blocks.append(third_in[r] - height * vert)
    y_forward(plan, blocks, 0, yf, out_ref)


def rates_kernel(
    plan, buf_ref, vertical_in, slope_ref, rate_ref, energy_ref, yi, out_ref,
    work_ref,
):
    y_inverse(plan, buf_ref, 1, yi, work_ref)
    N = plan.NYF
    for r in range(plan.R):
        vertical = vertical_in[r] + y_block(plan, work_ref, 0, r)
        lift = (1.0 + slope_ref[r]) * vertical
        out_ref[r, :N, :] = rate_ref[r] + lift
        out_ref[r, N : 2 * N, :] = energy_ref[r] + 0.5 * lift * vertical


def pools(rows_out, rows_in, cols_in, cols_out):
    def pool(shape, out_dim):
        i = lax.broadcasted_iota(jnp.int32, shape, out_dim)
        k = lax.broadcasted_iota(jnp.int32, shape, 1 - out_dim)
        return jnp.where((k >= COARSE * i) & (k < COARSE * (i + 1)), 1.0 / COARSE, 0.0).astype(BF16)

    return pool((rows_out, rows_in), 0), pool((cols_in, cols_out), 1)


def pooled(x, pool_y, pool_x):
    hi, lo = split(x)
    low = (x - hi.astype(F32) - lo.astype(F32)).astype(BF16)
    lines = dot(hi, pool_x) + (dot(lo, pool_x) + dot(low, pool_x))
    hi, lo = split(lines)
    low = (lines - hi.astype(F32) - lo.astype(F32)).astype(BF16)
    return dot(pool_y, hi) + (dot(pool_y, lo) + dot(pool_y, low))


def current_kernel(plan, in_ref, u_ref, v_ref):
    XH = plan.XC // COARSE
    for f, ref in enumerate((u_ref, v_ref)):
        for h in range(plan.Q):
            base = f * plan.NXC + h * XH
            ref[h * plan.NYC : (h + 1) * plan.NYC, :] = cat(
                [in_ref[r, :, base : base + XH] for r in range(plan.R)], 1
            )


def edges_kernel(in_ref, top_ref, bottom_ref, west_ref, east_ref):
    for ref in (top_ref, bottom_ref, west_ref, east_ref):
        ref[...] = jnp.zeros_like(ref)
    for q in range(3):
        x = in_ref[q, 0]
        top_ref[0, q : q + 1] = x[:1]
        bottom_ref[0, q : q + 1] = x[-1:]
        west_ref[0, q : q + 1] = jnp.transpose(x[:, :128])[:1]
        east_ref[0, q : q + 1] = jnp.transpose(x[:, -128:])[-1:]


def tile_kernel(
    plan, in_ref, height_ref, rate_ref, energy_ref, pressure_ref, top_ref, bottom_ref, west_ref, east_ref
):
    R, Q, XC, N = plan.R, plan.Q, plan.XC, plan.NYF
    for f, ref in enumerate((rate_ref, energy_ref)):
        for h in range(Q):
            ref[h * N : (h + 1) * N, :] = cat(
                [in_ref[r, f * N : (f + 1) * N, h * XC : (h + 1) * XC] for r in range(R)], 1
            )
    pool_y, pool_x = pools(plan.NYL // COARSE, plan.NYL, plan.NXL, plan.NXL // COARSE)
    pressure = GRAVITY * pooled(height_ref[...] + SURFACE_STEP * rate_ref[...], pool_y, pool_x)
    pressure_ref[...] = pressure
    top_ref[...] = pressure[:8]
    bottom_ref[...] = pressure[-8:]
    west_ref[...] = jnp.transpose(pressure[:, :128])[:8]
    east_ref[...] = jnp.transpose(pressure[:, -128:])[-8:]


def around(x, south, north, west, east):
    ny, nx = x.shape
    lane = lax.broadcasted_iota(jnp.int32, (ny, nx), 1)
    line = lax.broadcasted_iota(jnp.int32, (ny, nx), 0)
    return (
        jnp.where(lane == nx - 1, east, pltpu.roll(x, nx - 1, 1)),
        jnp.where(lane == 0, west, pltpu.roll(x, 1, 1)),
        jnp.where(line == ny - 1, north, pltpu.roll(x, ny - 1, 0)),
        jnp.where(line == 0, south, pltpu.roll(x, 1, 0)),
    )


def flow_kernel(
    decay_ref, prev_ref, cur_ref, next_ref, south_ref, north_ref, west_ref, east_ref,
    u_ref, v_ref, out_ref,
):
    level = pl.program_id(0)
    west_cols, east_cols = jnp.transpose(west_ref[0]), jnp.transpose(east_ref[0])
    top_u, top_v = u_ref[...], v_ref[...]
    is_top = level == 0

    def derivs(q, top):
        mid = cur_ref[q, 0]
        east, west, north, south = around(
            mid,
            south_ref[0, q : q + 1, :],
            north_ref[0, q : q + 1, :],
            west_cols[:, q : q + 1],
            east_cols[:, q : q + 1],
        )
        above = jnp.where(is_top, top, prev_ref[q, 0])
        below = next_ref[q, 0]
        lap = (east + west) + (north + south) + (above + below) - 6.0 * mid
        return mid, 0.5 * (east - west), 0.5 * (north - south), 0.5 * (above - below), lap

    u, u_dx, u_dy, u_dz, u_lap = derivs(0, top_u)
    v, v_dx, v_dy, v_dz, v_lap = derivs(1, top_v)
    w, w_dx, w_dy, w_dz, w_lap = derivs(2, jnp.zeros_like(top_u))
    drift_u = top_u * decay_ref[level, 0]
    drift_v = top_v * decay_ref[level, 0]
    vort_x = w_dy - v_dz
    vort_y = u_dz - w_dx
    vort_z = v_dx - u_dy

    def advance(mid, dx, dy, dz, lap, force):
        return mid + FLOW_STEP * (VISCOSITY * lap + force - (u * dx + v * dy + w * dz))

    out_ref[0, 0] = advance(u, u_dx, u_dy, u_dz, u_lap, drift_v * vort_z)
    out_ref[1, 0] = advance(v, v_dx, v_dy, v_dz, v_lap, -drift_u * vort_z)
    out_ref[2, 0] = advance(w, w_dx, w_dy, w_dz, w_lap, drift_u * vort_y - drift_v * vort_x)


def load_kernel(
    depth, decay_ref, flow_ref, pressure_ref, south_ref, north_ref, west_ref, east_ref,
    out_ref, x_ref, y_ref,
):
    step = pl.program_id(0)

    @pl.when(step == 0)
    def _():
        east, west, north, south = around(
            pressure_ref[...],
            south_ref[7:8, :],
            north_ref[0:1, :],
            jnp.transpose(west_ref[...])[:, 7:8],
            jnp.transpose(east_ref[...])[:, 0:1],
        )
        x_ref[...] = (0.5 * FLOW_STEP) * (east - west)
        y_ref[...] = (0.5 * FLOW_STEP) * (north - south)

    for l in range(depth):
        load = decay_ref[step * depth + l, 1]
        out_ref[0, l] = flow_ref[0, l] - load * x_ref[...]
        out_ref[1, l] = flow_ref[1, l] - load * y_ref[...]


def parts(table):
    hi = lax.reduce_precision(table, 8, 7)
    return hi.astype(BF16), (table - hi).astype(BF16)


def turns(numbers, places, total):
    numbers, places = lax.optimization_barrier((numbers, places))
    angle = (numbers * places % total).astype(F32) * (2.0 * math.pi / total)
    return lax.optimization_barrier((jnp.cos(angle), jnp.sin(angle)))


def table(coarse, fine, axis):
    return jnp.concatenate(
        [
            coarse[0] * fine[0] - coarse[1] * fine[1],
            coarse[1] * fine[0] + coarse[0] * fine[1],
        ],
        axis=axis,
    )


def make_tables(plan):
    ints = lambda count, *dims: jnp.expand_dims(jnp.arange(count, dtype=jnp.int32), dims)
    R, C, NY, NX = plan.R, plan.C, plan.NY, plan.NX
    coarse = turns(R * ints(plan.KY, 0, 2), ints(plan.NYL, 0, 1), NY)
    fine = turns(ints(R, 1, 2), ints(plan.NYL, 0, 1), NY)
    y_fwd = jnp.concatenate(parts(table(coarse, fine, 2)), axis=1)
    coarse = turns(R * ints(plan.KY, 0, 1), ints(plan.NYL, 0, 2), NY)
    fine = turns(ints(R, 1, 2), ints(plan.NYL, 0, 2), NY)
    y_inv = jnp.concatenate(parts(table(coarse, fine, 2)), axis=1)
    coarse = turns(C * ints(plan.J, 0, 1), ints(plan.NXL, 0, 2), NX)
    fine = turns(ints(C, 1, 2), ints(plan.NXL, 0, 2), NX)
    x_fwd = parts(table(coarse, fine, 2))
    return y_fwd, y_inv, x_fwd


def call(kernel, name, outs, args, smem=0, tables=(), work=(), cost=4.0, limit=12):
    vmem = pl.BlockSpec(memory_space=pltpu.VMEM)
    args = [*args, *tables]
    return pl.pallas_call(
        kernel,
        out_shape=[jax.ShapeDtypeStruct(o, F32) for o in outs],
        in_specs=[pl.BlockSpec(memory_space=pltpu.SMEM)] * smem + [vmem] * (len(args) - smem),
        out_specs=[vmem] * len(outs),
        scratch_shapes=[pltpu.VMEM(w, F32) for w in work],
        compiler_params=pltpu.CompilerParams(vmem_limit_bytes=limit * MIB),
        cost_estimate=priced(cost),
        name=name,
    )(*args)


def priced(microseconds):
    return pl.CostEstimate(
        flops=int(microseconds * 3e8), bytes_accessed=int(microseconds * 1e6), transcendentals=0
    )


def exchange(x, axes):
    return lax.all_to_all(x, axes, split_axis=0, concat_axis=0, tiled=True)


def shift(x, axis, step):
    peers = lax.axis_size(axis)
    return lax.ppermute(x, axis, [(i, (i + step) % peers) for i in range(peers)])


def from_neighbours(top, bottom, west, east):
    return (
        shift(bottom, "row", 1),
        shift(top, "row", -1),
        shift(east, "col", 1),
        shift(west, "col", -1),
    )


def local(surface_height, surface_potential, velocity):
    plan = Plan(lax.axis_size("row"), lax.axis_size("col"), surface_height.shape)
    R, C, M, W, N, L2 = plan.R, plan.C, plan.M, plan.W, plan.NYF, plan.L2
    bind = lambda kernel, *rest: functools.partial(kernel, plan, *rest)
    both = ("row", "col")
    pencil = (R, N, W)
    work = lambda f: (R // 2 + 1, plan.NYL, f * L2)
    spec = lambda f: (plan.PEERS, f * M, L2)

    (packed,) = call(
        bind(pack_kernel), "pack", [(R, 2 * N, W)], [surface_potential, surface_height]
    )
    packed = exchange(packed, "row")

    levels, ny, nx = velocity.shape[1:]
    depth = 4 if levels % 4 == 0 else 1
    block = (3, 1, ny, nx)
    at = lambda step: pl.BlockSpec(
        block, lambda l: (0, jnp.clip(l + step, 0, levels - 1), 0, 0)
    )
    whole = lambda x: pl.BlockSpec(x.shape, lambda l: (0,) * x.ndim)
    per_level = lambda length: pl.BlockSpec((1, 8, length), lambda l: (l, 0, 0))
    smem = pl.BlockSpec(memory_space=pltpu.SMEM)
    edge_specs = [per_level(nx)] * 2 + [per_level(ny)] * 2
    edges = pl.pallas_call(
        edges_kernel,
        grid=(levels,),
        out_shape=[jax.ShapeDtypeStruct((levels, 8, n), F32) for n in (nx, nx, ny, ny)],
        in_specs=[at(0)],
        out_specs=edge_specs,
        compiler_params=pltpu.CompilerParams(vmem_limit_bytes=16 * MIB),
        cost_estimate=priced(5.0),
        name="edges",
    )(velocity)
    edges = from_neighbours(*edges)
    mid = jnp.arange(levels, dtype=F32) + 0.5
    decay = jnp.stack([jnp.exp(-2.0 * DECAY_RATE * mid), jnp.exp(-DECAY_RATE * mid)], axis=1)

    y_fwd, y_inv, x_tables = make_tables(plan)
    place = jnp.stack([lax.axis_index("row"), lax.axis_index("col") * M]).astype(jnp.int32)

    def x_stage(buf, sources, wanted):
        outs = len(wanted)
        slots = C // 2 + 1 + max(0, (C - 1) // 2)
        (out,) = call(
            bind(x_kernel, sources, wanted),
            "x%d" % outs,
            [spec(outs)],
            [place, buf],
            smem=1,
            tables=x_tables,
            work=[(slots, 2 * outs * M, plan.NXL)],
            cost=3.0 + outs,
            limit=10 + 2 * outs,
        )
        return out

    first, height = call(bind(first_kernel), "y0", [spec(2), pencil], [packed], tables=[y_fwd])
    first = exchange(first, both)
    vert = exchange(x_stage(first, (0,), ((0, 1),)), both)
    rest = exchange(
        x_stage(first, (0, 1), ((0, 2), (0, 3), (0, "dx"), (0, "dy"), (1, "dx"), (1, "dy"))),
        both,
    )
    second, vert = call(
        bind(second_kernel), "y1", [spec(1), pencil], [vert, height],
        tables=[y_inv, y_fwd], work=[work(1)],
    )
    second = exchange(second, both)
    vertical, third, slope, rate, energy, coarse = call(
        bind(fields_kernel), "y6", [pencil] * 5 + [(R, plan.NYC, 2 * plan.NXC)],
        [rest, height, vert], tables=[y_inv], work=[work(6)], cost=9.0, limit=20,
    )
    second, edges = lax.optimization_barrier((x_stage(second, (0,), ((0, 1), (0, 2))), edges))
    second = exchange(second, both)
    current = exchange(coarse, "row")
    surface_u, surface_v = call(bind(current_kernel), "currents", [(ny, nx)] * 2, [current])

    flow = pl.pallas_call(
        flow_kernel,
        grid=(levels,),
        out_shape=jax.ShapeDtypeStruct(velocity.shape, F32),
        in_specs=[smem, at(-1), at(0), at(1)]
        + edge_specs
        + [whole(x) for x in (surface_u, surface_v)],
        out_specs=at(0),
        compiler_params=pltpu.CompilerParams(vmem_limit_bytes=16 * MIB),
        cost_estimate=priced(19.0),
        name="flow",
    )(decay, velocity, velocity, velocity, *edges, surface_u, surface_v)

    last, vertical = call(
        bind(third_kernel), "y2", [spec(1), pencil], [second, height, vertical, third],
        tables=[y_inv, y_fwd], work=[work(2)],
    )
    last = exchange(x_stage(exchange(last, both), (0,), ((0, 1),)), both)
    (rates,) = call(
        bind(rates_kernel), "y3", [(R, 2 * N, W)], [last, vertical, slope, rate, energy],
        tables=[y_inv], work=[work(1)],
    )
    rates, flow = lax.optimization_barrier((exchange(rates, "row"), flow))
    tile = surface_height.shape
    height_rate, potential_rate, pressure, *sides = call(
        bind(tile_kernel), "tile", [tile, tile, (ny, nx)] + [(8, nx)] * 2 + [(8, ny)] * 2,
        [rates, surface_height],
    )
    sides = from_neighbours(*sides)
    pair = pl.BlockSpec((2, depth, ny, nx), lambda l: (0, l, 0, 0))
    velocity_next = pl.pallas_call(
        functools.partial(load_kernel, depth),
        grid=(levels // depth,),
        out_shape=jax.ShapeDtypeStruct(velocity.shape, F32),
        in_specs=[smem, pair] + [whole(x) for x in (pressure, *sides)],
        out_specs=pair,
        scratch_shapes=[pltpu.VMEM((ny, nx), F32)] * 2,
        input_output_aliases={1: 0},
        compiler_params=pltpu.CompilerParams(vmem_limit_bytes=16 * MIB),
        cost_estimate=priced(4.0),
        name="load",
    )(decay, flow, pressure, *sides)
    return height_rate, potential_rate, velocity_next


def solution(mesh):
    placed = (P("row", "col"), P("row", "col"), P(None, None, "row", "col"))
    return jax.shard_map(
        local,
        mesh=mesh,
        in_specs=placed,
        out_specs=placed,
        check_vma=False,
    )
```

```python
import functools
import math

import jax
import jax.numpy as jnp
from jax import lax
from jax.experimental import pallas as pl
from jax.experimental.pallas import tpu as pltpu
from jax.sharding import PartitionSpec as P

COARSE = 2
GRAVITY = 1.0
SURFACE_STEP = 0.05
FLOW_STEP = 0.5
VISCOSITY = 0.2
DECAY_RATE = 0.05

F32 = jnp.float32
BF16 = jnp.bfloat16
MIB = 1024 * 1024


def round_up(value, step):
    return -(-value // step) * step


class Plan:
    def __init__(self, rows, cols, tile):
        self.R, self.C = rows, cols
        self.NYL, self.NXL = tile
        self.NY, self.NX = rows * self.NYL, cols * self.NXL
        self.XC = self.NXL // rows
        self.Q = max(1, 128 // self.XC)
        self.NYF = self.NYL // self.Q
        self.W = self.Q * self.XC
        self.KEPT_Y = self.NY // 3 + 1
        self.KEPT_X = self.NX // 3 + 1
        self.M = round_up(-(-(-(-self.KEPT_Y // rows)) // cols), 8)
        self.KY = cols * self.M
        self.J = round_up(-(-self.KEPT_X // cols), 128)
        self.L2 = 2 * self.XC
        self.PEERS = rows * cols
        self.NYC, self.NXC = self.NYF // COARSE, self.W // COARSE


def split(x):
    hi = x.astype(BF16)
    return hi, (x - hi.astype(F32)).astype(BF16)


def dot(a, b, flipped=False):
    dims = (((1,), (1 if flipped else 0,)), ((), ()))
    return lax.dot_general(a, b, dims, preferred_element_type=F32)


def cat(parts, axis):
    return parts[0] if len(parts) == 1 else jnp.concatenate(parts, axis=axis)


def turn(numer, denom):
    numer %= denom
    exact = {0: (1.0, 0.0), 1: (0.0, 1.0), 2: (-1.0, 0.0), 3: (0.0, -1.0)}
    if 4 * numer % denom == 0:
        return exact[4 * numer // denom]
    angle = 2.0 * math.pi * numer / denom
    return math.cos(angle), math.sin(angle)


def combine(terms):
    total = None
    for factor, value in terms:
        if factor == 0.0:
            continue
        if total is None:
            total = value if factor == 1.0 else (-value if factor == -1.0 else factor * value)
        elif factor == 1.0:
            total = total + value
        elif factor == -1.0:
            total = total - value
        else:
            total = total + factor * value
    return total


def mirrored(index, count):
    if index == 0 or 2 * index == count:
        return ((index, 1.0),)
    return ((index, 1.0), (count - index, -1.0))


def unfold(x, plan):
    return cat([x[:, h * plan.XC : (h + 1) * plan.XC] for h in range(plan.Q)], 0)


def fold(x, plan):
    return cat([x[h * plan.NYF : (h + 1) * plan.NYF] for h in range(plan.Q)], 1)


def swap_halves(x, half):
    if 2 * half == 128:
        return pltpu.roll(x, half, 1)
    return jnp.concatenate([x[:, half:], x[:, :half]], axis=1)


def table_rows(table, rhs):
    rows = table.shape[0] // 2
    both = dot(table, rhs[0])
    return both[:rows] + (both[rows:] + dot(table[:rows], rhs[1]))


def y_forward(plan, blocks, field, tab, out_ref):
    for k0 in range(plan.R // 2 + 1):
        even = combine([(turn(k0 * r, plan.R)[0], blocks[r]) for r in range(plan.R)])
        odd = combine([(turn(k0 * r, plan.R)[1], blocks[r]) for r in range(plan.R)])
        even = split(unfold(even, plan))
        if odd is None:
            odd = tuple(jnp.zeros_like(e) for e in even)
        else:
            odd = split(unfold(odd, plan))
        for k, sign in mirrored(k0, plan.R):
            if sign > 0:
                pos, neg = odd, [-o for o in odd]
            else:
                pos, neg = [-o for o in odd], odd
            rhs = [
                jnp.concatenate(
                    [
                        jnp.concatenate([even[i], pos[i]], axis=1),
                        jnp.concatenate([neg[i], even[i]], axis=1),
                    ],
                    axis=0,
                )
                for i in range(2)
            ]
            lines = table_rows(tab[k], rhs)
            for c in range(plan.C):
                out_ref[k * plan.C + c, field * plan.M : (field + 1) * plan.M, :] = lines[
                    c * plan.M : (c + 1) * plan.M
                ]


def y_inverse(plan, buf_ref, fields, tab, work_ref):
    L2, M, C = plan.L2, plan.M, plan.C
    lane = lax.broadcasted_iota(jnp.int32, (1, L2), 1)
    flip = jnp.where(lane < plan.XC, 1.0, -1.0).astype(F32)
    for k0 in range(plan.R // 2 + 1):
        total = None
        for k, sign in mirrored(k0, plan.R):
            tops, bottoms = [], []
            for f in range(fields):
                lines = cat(
                    [buf_ref[k * C + c, f * M : (f + 1) * M, :] for c in range(C)], 0
                )
                tops.append(lines)
                bottoms.append(swap_halves(lines, plan.XC) * flip)
            rhs = split(jnp.concatenate([cat(tops, 1), cat(bottoms, 1)], axis=0))
            part = table_rows(tab[k], rhs)
            if sign > 0:
                total = part
            else:
                total = total + part * cat([flip] * fields, 1)
        work_ref[k0] = total


def y_block(plan, work_ref, field, r):
    L2 = plan.L2
    lane = lax.broadcasted_iota(jnp.int32, (1, L2), 1)
    total = None
    for k0 in range(plan.R // 2 + 1):
        c, s = turn(k0 * r, plan.R)
        factor = jnp.where(lane < plan.XC, c, s).astype(F32)
        part = work_ref[k0, :, field * L2 : (field + 1) * L2] * factor
        total = part if total is None else total + part
    if L2 == 128 and plan.Q == 2:
        both = total + pltpu.roll(total, plan.XC, 1)
        return jnp.where(lane < plan.XC, both[: plan.NYF], both[plan.NYF :])
    return fold(total[:, : plan.XC] + total[:, plan.XC :], plan)


def pack_kernel(plan, potential_ref, height_ref, out_ref):
    for r in range(plan.R):
        for f, ref in enumerate((potential_ref, height_ref)):
            out_ref[r, f * plan.NYF : (f + 1) * plan.NYF, :] = fold(
                ref[:, r * plan.XC : (r + 1) * plan.XC], plan
            )


def first_kernel(plan, in_ref, yf, out_ref, height_ref):
    for f in range(2):
        blocks = [in_ref[r, f * plan.NYF : (f + 1) * plan.NYF, :] for r in range(plan.R)]
        y_forward(plan, blocks, f, yf, out_ref)
    for r in range(plan.R):
        height_ref[r] = in_ref[r, plan.NYF :, :]


def stacked(pair, table_hi, table_lo, flipped=False):
    hi = cat([p[0] for p in pair], 0)
    lo = cat([p[1] for p in pair], 0)
    rows = hi.shape[0]
    both = dot(jnp.concatenate([hi, lo], axis=0), table_hi, flipped)
    total = both[:rows] + (both[rows:] + dot(hi, table_lo, flipped))
    rows = pair[0][0].shape[0]
    return [total[i * rows : (i + 1) * rows] for i in range(len(pair))]


def x_kernel(
    plan, sources, wanted, place_ref, in_ref, fh, fl, out_ref, u_ref,
):
    R, C, M, J, XC, NXL = plan.R, plan.C, plan.M, plan.J, plan.XC, plan.NXL
    fields, outs = len(sources), len(wanted)
    rows = fields * M
    lines = []
    for c in range(C):
        parts_of = []
        for h in range(2):
            for f in sources:
                parts_of.append(
                    cat(
                        [
                            in_ref[r * C + c, f * M : (f + 1) * M, h * XC : (h + 1) * XC]
                            for r in range(R)
                        ],
                        1,
                    )
                )
        lines.append(jnp.concatenate(parts_of, axis=0))
    row_k0, row_k1 = place_ref[0], place_ref[1]
    ky_index = R * (row_k1 + lax.broadcasted_iota(jnp.int32, (M, J), 0)) + row_k0
    ky = ky_index.astype(F32) * (2.0 * math.pi / plan.NY)
    y_weight = jnp.where(
        ky_index == 0, 1.0, jnp.where(ky_index < plan.KEPT_Y, 2.0, 0.0)
    ).astype(F32)
    slot = 0
    slots = []
    for j0 in range(C // 2 + 1):
        pair = [split(combine([(turn(j0 * c, C)[0], lines[c]) for c in range(C)]))]
        odd = combine([(turn(j0 * c, C)[1], lines[c]) for c in range(C)])
        if odd is not None:
            pair.append(split(odd))
        u_sum = v_sum = None
        for j, sign in mirrored(j0, C):
            found = stacked(pair, fh[j], fl[j])
            p_all, q_all = found[0][:, :J], found[0][:, J:]
            if odd is not None:
                p_all = p_all - sign * found[1][:, J:]
                q_all = q_all + sign * found[1][:, :J]
            kx_index = C * lax.broadcasted_iota(jnp.int32, (M, J), 1) + j
            kx = kx_index.astype(F32) * (2.0 * math.pi / plan.NX)
            x_weight = jnp.where(
                kx_index == 0, 1.0, jnp.where(kx_index < plan.KEPT_X, 2.0, 0.0)
            ).astype(F32)
            weight = x_weight * y_weight * (1.0 / (plan.NX * plan.NY))
            size = jnp.sqrt(kx * kx + ky * ky)
            coef = []
            for f in range(fields):
                top, low = slice(f * M, (f + 1) * M), slice(rows + f * M, rows + (f + 1) * M)
                coef.append(
                    (
                        p_all[top] * weight,
                        q_all[top] * weight,
                        p_all[low] * weight,
                        q_all[low] * weight,
                    )
                )
            tops, lows = [], []
            for f, kind in wanted:
                cc, cs, sc, ss = coef[f]
                if kind == "dx":
                    new = (kx * cs, -kx * cc, kx * ss, -kx * sc)
                elif kind == "dy":
                    new = (ky * sc, ky * ss, -ky * cc, -ky * cs)
                else:
                    factor = size
                    for _ in range(kind - 1):
                        factor = factor * size
                    new = (factor * cc, factor * cs, factor * sc, factor * ss)
                tops.append((new[0], new[1]))
                lows.append((new[2], new[3]))
            p_new = split(cat([t[0] for t in tops] + [t[0] for t in lows], 0))
            q_new = split(cat([t[1] for t in tops] + [t[1] for t in lows], 0))
            pair_back = [[jnp.concatenate([p_new[i], q_new[i]], axis=1) for i in range(2)]]
            if odd is not None:
                pair_back.append(
                    [jnp.concatenate([q_new[i], -p_new[i]], axis=1) for i in range(2)]
                )
            found = stacked(pair_back, fh[j], fl[j], True)
            u_sum = found[0] if u_sum is None else u_sum + found[0]
            if odd is not None:
                v_sum = found[1] if v_sum is None else v_sum - found[1]
        u_ref[slot] = u_sum
        slots.append((j0, slot, None if v_sum is None else slot + 1))
        if v_sum is not None:
            u_ref[slot + 1] = v_sum
        slot += 1 if v_sum is None else 2
    half = outs * M
    for c in range(C):
        terms = []
        for j0, u_slot, v_slot in slots:
            cs, sn = turn(j0 * c, C)
            terms.append((cs, u_slot))
            if v_slot is not None:
                terms.append((sn, v_slot))
        for r in range(0, R):
            lanes = slice(r * XC, (r + 1) * XC)
            top = combine([(a, u_ref[s, :half, lanes]) for a, s in terms if a != 0.0])
            low = combine([(a, u_ref[s, half:, lanes]) for a, s in terms if a != 0.0])
            out_ref[r * C + c] = jnp.concatenate([top, low], axis=1)


def second_kernel(
    plan, buf_ref, height_ref, yi, yf, out_ref, vert_ref, work_ref
):
    y_inverse(plan, buf_ref, 1, yi, work_ref)
    blocks = []
    for r in range(plan.R):
        vert = y_block(plan, work_ref, 0, r)
        vert_ref[r] = vert
        blocks.append(-height_ref[r] * vert)
    y_forward(plan, blocks, 0, yf, out_ref)


def fields_kernel(
    plan, buf_ref, height_ref, vert_ref, yi,
    vertical_ref, third_ref, slope_ref, rate_ref, energy_ref, coarse_ref,
    work_ref,
):
    y_inverse(plan, buf_ref, 6, yi, work_ref)
    pool_y, pool_x = pools(plan.NYC, plan.NYF, plan.W, plan.NXC)
    for r in range(plan.R):
        height = height_ref[r]
        curve, cube, pot_dx, pot_dy, height_dx, height_dy = [
            y_block(plan, work_ref, f, r) for f in range(6)
        ]
        square = 0.5 * height * height
        vertical_ref[r] = vert_ref[r] + height * curve + square * cube
        third_ref[r] = -square * curve
        slope_ref[r] = height_dx * height_dx + height_dy * height_dy
        rate_ref[r] = -(height_dx * pot_dx + height_dy * pot_dy)
        energy_ref[r] = -GRAVITY * height - 0.5 * (pot_dx * pot_dx + pot_dy * pot_dy)
        coarse_ref[r] = jnp.concatenate(
            [pooled(pot_dx, pool_y, pool_x), pooled(pot_dy, pool_y, pool_x)], axis=1
        )


def third_kernel(
    plan, buf_ref, height_ref, vertical_in, third_in, yi, yf, out_ref, vertical_ref,
    work_ref,
):
    y_inverse(plan, buf_ref, 2, yi, work_ref)
    blocks = []
    for r in range(plan.R):
        height = height_ref[r]
        vert, curve = [y_block(plan, work_ref, f, r) for f in range(2)]
        vertical_ref[r] = vertical_in[r] + vert + height * curve
        blocks.append(third_in[r] - height * vert)
    y_forward(plan, blocks, 0, yf, out_ref)


def rates_kernel(
    plan, buf_ref, vertical_in, slope_ref, rate_ref, energy_ref, yi, out_ref,
    work_ref,
):
    y_inverse(plan, buf_ref, 1, yi, work_ref)
    N = plan.NYF
    for r in range(plan.R):
        vertical = vertical_in[r] + y_block(plan, work_ref, 0, r)
        lift = (1.0 + slope_ref[r]) * vertical
        out_ref[r, :N, :] = rate_ref[r] + lift
        out_ref[r, N : 2 * N, :] = energy_ref[r] + 0.5 * lift * vertical


def pools(rows_out, rows_in, cols_in, cols_out):
    def pool(shape, out_dim):
        i = lax.broadcasted_iota(jnp.int32, shape, out_dim)
        k = lax.broadcasted_iota(jnp.int32, shape, 1 - out_dim)
        return jnp.where((k >= COARSE * i) & (k < COARSE * (i + 1)), 1.0 / COARSE, 0.0).astype(BF16)

    return pool((rows_out, rows_in), 0), pool((cols_in, cols_out), 1)


def pooled(x, pool_y, pool_x):
    hi, lo = split(x)
    low = (x - hi.astype(F32) - lo.astype(F32)).astype(BF16)
    lines = dot(hi, pool_x) + (dot(lo, pool_x) + dot(low, pool_x))
    hi, lo = split(lines)
    low = (lines - hi.astype(F32) - lo.astype(F32)).astype(BF16)
    return dot(pool_y, hi) + (dot(pool_y, lo) + dot(pool_y, low))


def current_kernel(plan, in_ref, u_ref, v_ref):
    XH = plan.XC // COARSE
    for f, ref in enumerate((u_ref, v_ref)):
        for h in range(plan.Q):
            base = f * plan.NXC + h * XH
            ref[h * plan.NYC : (h + 1) * plan.NYC, :] = cat(
                [in_ref[r, :, base : base + XH] for r in range(plan.R)], 1
            )


def edges_kernel(in_ref, top_ref, bottom_ref, west_ref, east_ref):
    for ref in (top_ref, bottom_ref, west_ref, east_ref):
        ref[...] = jnp.zeros_like(ref)
    for q in range(3):
        x = in_ref[q, 0]
        top_ref[0, q : q + 1] = x[:1]
        bottom_ref[0, q : q + 1] = x[-1:]
        west_ref[0, q : q + 1] = jnp.transpose(x[:, :128])[:1]
        east_ref[0, q : q + 1] = jnp.transpose(x[:, -128:])[-1:]


def tile_kernel(
    plan, in_ref, height_ref, rate_ref, energy_ref, pressure_ref, top_ref, bottom_ref, west_ref, east_ref
):
    R, Q, XC, N = plan.R, plan.Q, plan.XC, plan.NYF
    for f, ref in enumerate((rate_ref, energy_ref)):
        for h in range(Q):
            ref[h * N : (h + 1) * N, :] = cat(
                [in_ref[r, f * N : (f + 1) * N, h * XC : (h + 1) * XC] for r in range(R)], 1
            )
    pool_y, pool_x = pools(plan.NYL // COARSE, plan.NYL, plan.NXL, plan.NXL // COARSE)
    pressure = GRAVITY * pooled(height_ref[...] + SURFACE_STEP * rate_ref[...], pool_y, pool_x)
    pressure_ref[...] = pressure
    top_ref[...] = pressure[:8]
    bottom_ref[...] = pressure[-8:]
    west_ref[...] = jnp.transpose(pressure[:, :128])[:8]
    east_ref[...] = jnp.transpose(pressure[:, -128:])[-8:]


def around(x, south, north, west, east):
    ny, nx = x.shape
    lane = lax.broadcasted_iota(jnp.int32, (ny, nx), 1)
    line = lax.broadcasted_iota(jnp.int32, (ny, nx), 0)
    return (
        jnp.where(lane == nx - 1, east, pltpu.roll(x, nx - 1, 1)),
        jnp.where(lane == 0, west, pltpu.roll(x, 1, 1)),
        jnp.where(line == ny - 1, north, pltpu.roll(x, ny - 1, 0)),
        jnp.where(line == 0, south, pltpu.roll(x, 1, 0)),
    )


def flow_kernel(
    decay_ref, prev_ref, cur_ref, next_ref, south_ref, north_ref, west_ref, east_ref,
    u_ref, v_ref, out_ref,
):
    level = pl.program_id(0)
    west_cols, east_cols = jnp.transpose(west_ref[0]), jnp.transpose(east_ref[0])
    top_u, top_v = u_ref[...], v_ref[...]
    is_top = level == 0

    def differences(q, top):
        mid = cur_ref[q, 0]
        east, west, north, south = around(
            mid,
            south_ref[0, q : q + 1, :],
            north_ref[0, q : q + 1, :],
            west_cols[:, q : q + 1],
            east_cols[:, q : q + 1],
        )
        above = jnp.where(is_top, top, prev_ref[q, 0])
        below = next_ref[q, 0]
        total = (east + west) + (north + south) + (above + below)
        return mid, east - west, north - south, above - below, total

    u, u_dx, u_dy, u_dz, u_sum = differences(0, top_u)
    v, v_dx, v_dy, v_dz, v_sum = differences(1, top_v)
    w, w_dx, w_dy, w_dz, w_sum = differences(2, 0.0)
    half = 0.5 * FLOW_STEP
    fall = half * decay_ref[level, 0]
    drift_u, drift_v = top_u * fall, top_v * fall
    vort_x = w_dy - v_dz
    vort_y = u_dz - w_dx
    vort_z = v_dx - u_dy
    spread_by = FLOW_STEP * VISCOSITY
    half_u, half_v, half_w = half * u, half * v, half * w

    def advance(mid, dx, dy, dz, total, force):
        carried = half_u * dx + half_v * dy + half_w * dz
        return (1.0 - 6.0 * spread_by) * mid + spread_by * total + (force - carried)

    out_ref[0, 0] = advance(u, u_dx, u_dy, u_dz, u_sum, drift_v * vort_z)
    out_ref[1, 0] = advance(v, v_dx, v_dy, v_dz, v_sum, -drift_u * vort_z)
    out_ref[2, 0] = advance(w, w_dx, w_dy, w_dz, w_sum, drift_u * vort_y - drift_v * vort_x)


def load_kernel(
    depth, decay_ref, flow_ref, pressure_ref, south_ref, north_ref, west_ref, east_ref,
    out_ref, x_ref, y_ref,
):
    step = pl.program_id(0)

    @pl.when(step == 0)
    def _():
        east, west, north, south = around(
            pressure_ref[...],
            south_ref[7:8, :],
            north_ref[0:1, :],
            jnp.transpose(west_ref[...])[:, 7:8],
            jnp.transpose(east_ref[...])[:, 0:1],
        )
        x_ref[...] = (0.5 * FLOW_STEP) * (east - west)
        y_ref[...] = (0.5 * FLOW_STEP) * (north - south)

    for l in range(depth):
        load = decay_ref[step * depth + l, 1]
        out_ref[0, l] = flow_ref[0, l] - load * x_ref[...]
        out_ref[1, l] = flow_ref[1, l] - load * y_ref[...]


def parts(table):
    hi = lax.reduce_precision(table, 8, 7)
    return hi.astype(BF16), (table - hi).astype(BF16)


def turns(numbers, places, total):
    numbers, places = lax.optimization_barrier((numbers, places))
    angle = (numbers * places % total).astype(F32) * (2.0 * math.pi / total)
    return lax.optimization_barrier((jnp.cos(angle), jnp.sin(angle)))


def table(coarse, fine, axis):
    return jnp.concatenate(
        [
            coarse[0] * fine[0] - coarse[1] * fine[1],
            coarse[1] * fine[0] + coarse[0] * fine[1],
        ],
        axis=axis,
    )


def make_tables(plan):
    ints = lambda count, *dims: jnp.expand_dims(jnp.arange(count, dtype=jnp.int32), dims)
    R, C, NY, NX = plan.R, plan.C, plan.NY, plan.NX
    coarse = turns(R * ints(plan.KY, 0, 2), ints(plan.NYL, 0, 1), NY)
    fine = turns(ints(R, 1, 2), ints(plan.NYL, 0, 1), NY)
    y_fwd = jnp.concatenate(parts(table(coarse, fine, 2)), axis=1)
    coarse, fine = [tuple(jnp.swapaxes(x, 1, 2) for x in t) for t in (coarse, fine)]
    y_inv = jnp.concatenate(parts(table(coarse, fine, 2)), axis=1)
    coarse = turns(C * ints(plan.J, 0, 1), ints(plan.NXL, 0, 2), NX)
    fine = turns(ints(C, 1, 2), ints(plan.NXL, 0, 2), NX)
    x_fwd = parts(table(coarse, fine, 2))
    return y_fwd, y_inv, x_fwd


def call(kernel, name, outs, args, smem=0, tables=(), work=(), cost=4.0, limit=12):
    vmem = pl.BlockSpec(memory_space=pltpu.VMEM)
    args = [*args, *tables]
    return pl.pallas_call(
        kernel,
        out_shape=[jax.ShapeDtypeStruct(o, F32) for o in outs],
        in_specs=[pl.BlockSpec(memory_space=pltpu.SMEM)] * smem + [vmem] * (len(args) - smem),
        out_specs=[vmem] * len(outs),
        scratch_shapes=[pltpu.VMEM(w, F32) for w in work],
        compiler_params=pltpu.CompilerParams(vmem_limit_bytes=limit * MIB),
        cost_estimate=priced(cost),
        name=name,
    )(*args)


def priced(microseconds):
    return pl.CostEstimate(
        flops=int(microseconds * 3e8), bytes_accessed=int(microseconds * 1e6), transcendentals=0
    )


def exchange(x, axes):
    return lax.all_to_all(x, axes, split_axis=0, concat_axis=0, tiled=True)


def shift(x, axis, step):
    peers = lax.axis_size(axis)
    return lax.ppermute(x, axis, [(i, (i + step) % peers) for i in range(peers)])


def from_neighbours(top, bottom, west, east):
    return (
        shift(bottom, "row", 1),
        shift(top, "row", -1),
        shift(east, "col", 1),
        shift(west, "col", -1),
    )


def local(surface_height, surface_potential, velocity):
    plan = Plan(lax.axis_size("row"), lax.axis_size("col"), surface_height.shape)
    R, C, M, W, N, L2 = plan.R, plan.C, plan.M, plan.W, plan.NYF, plan.L2
    bind = lambda kernel, *rest: functools.partial(kernel, plan, *rest)
    both = ("row", "col")
    pencil = (R, N, W)
    work = lambda f: (R // 2 + 1, plan.NYL, f * L2)
    spec = lambda f: (plan.PEERS, f * M, L2)

    (packed,) = call(
        bind(pack_kernel), "pack", [(R, 2 * N, W)], [surface_potential, surface_height]
    )
    packed = exchange(packed, "row")

    levels, ny, nx = velocity.shape[1:]
    depth = 2 if levels % 2 == 0 else 1
    block = (3, 1, ny, nx)
    at = lambda step: pl.BlockSpec(
        block, lambda l: (0, jnp.clip(l + step, 0, levels - 1), 0, 0)
    )
    whole = lambda x: pl.BlockSpec(x.shape, lambda l: (0,) * x.ndim)
    per_level = lambda length: pl.BlockSpec((1, 8, length), lambda l: (l, 0, 0))
    smem = pl.BlockSpec(memory_space=pltpu.SMEM)
    edge_specs = [per_level(nx)] * 2 + [per_level(ny)] * 2
    edges = pl.pallas_call(
        edges_kernel,
        grid=(levels,),
        out_shape=[jax.ShapeDtypeStruct((levels, 8, n), F32) for n in (nx, nx, ny, ny)],
        in_specs=[at(0)],
        out_specs=edge_specs,
        compiler_params=pltpu.CompilerParams(vmem_limit_bytes=16 * MIB),
        cost_estimate=priced(5.0),
        name="edges",
    )(velocity)
    edges = from_neighbours(*edges)
    mid = jnp.arange(levels, dtype=F32) + 0.5
    decay = jnp.stack([jnp.exp(-2.0 * DECAY_RATE * mid), jnp.exp(-DECAY_RATE * mid)], axis=1)

    y_fwd, y_inv, x_tables = make_tables(plan)
    place = jnp.stack([lax.axis_index("row"), lax.axis_index("col") * M]).astype(jnp.int32)

    def x_stage(buf, sources, wanted):
        outs = len(wanted)
        slots = C // 2 + 1 + max(0, (C - 1) // 2)
        (out,) = call(
            bind(x_kernel, sources, wanted),
            "x%d" % outs,
            [spec(outs)],
            [place, buf],
            smem=1,
            tables=x_tables,
            work=[(slots, 2 * outs * M, plan.NXL)],
            cost=3.0 + outs,
            limit=10 + 2 * outs,
        )
        return out

    first, height = call(bind(first_kernel), "y0", [spec(2), pencil], [packed], tables=[y_fwd])
    first = exchange(first, both)
    vert = exchange(x_stage(first, (0,), ((0, 1),)), both)
    rest = exchange(
        x_stage(first, (0, 1), ((0, 2), (0, 3), (0, "dx"), (0, "dy"), (1, "dx"), (1, "dy"))),
        both,
    )
    second, vert = call(
        bind(second_kernel), "y1", [spec(1), pencil], [vert, height],
        tables=[y_inv, y_fwd], work=[work(1)],
    )
    second = exchange(second, both)
    vertical, third, slope, rate, energy, coarse = call(
        bind(fields_kernel), "y6", [pencil] * 5 + [(R, plan.NYC, 2 * plan.NXC)],
        [rest, height, vert], tables=[y_inv], work=[work(6)], cost=9.0, limit=20,
    )
    second, edges = lax.optimization_barrier((x_stage(second, (0,), ((0, 1), (0, 2))), edges))
    second = exchange(second, both)
    current = exchange(coarse, "row")
    surface_u, surface_v = call(bind(current_kernel), "currents", [(ny, nx)] * 2, [current])

    flow = pl.pallas_call(
        flow_kernel,
        grid=(levels,),
        out_shape=jax.ShapeDtypeStruct(velocity.shape, F32),
        in_specs=[smem, at(-1), at(0), at(1)]
        + edge_specs
        + [whole(x) for x in (surface_u, surface_v)],
        out_specs=at(0),
        compiler_params=pltpu.CompilerParams(vmem_limit_bytes=16 * MIB),
        cost_estimate=priced(19.0),
        name="flow",
    )(decay, velocity, velocity, velocity, *edges, surface_u, surface_v)

    last, vertical = call(
        bind(third_kernel), "y2", [spec(1), pencil], [second, height, vertical, third],
        tables=[y_inv, y_fwd], work=[work(2)],
    )
    last = exchange(x_stage(exchange(last, both), (0,), ((0, 1),)), both)
    (rates,) = call(
        bind(rates_kernel), "y3", [(R, 2 * N, W)], [last, vertical, slope, rate, energy],
        tables=[y_inv], work=[work(1)],
    )
    rates, flow = lax.optimization_barrier((exchange(rates, "row"), flow))
    tile = surface_height.shape
    height_rate, potential_rate, pressure, *sides = call(
        bind(tile_kernel), "tile", [tile, tile, (ny, nx)] + [(8, nx)] * 2 + [(8, ny)] * 2,
        [rates, surface_height],
    )
    sides = from_neighbours(*sides)
    pair = pl.BlockSpec((2, depth, ny, nx), lambda l: (0, l, 0, 0))
    velocity_next = pl.pallas_call(
        functools.partial(load_kernel, depth),
        grid=(levels // depth,),
        out_shape=jax.ShapeDtypeStruct(velocity.shape, F32),
        in_specs=[smem, pair] + [whole(x) for x in (pressure, *sides)],
        out_specs=pair,
        scratch_shapes=[pltpu.VMEM((ny, nx), F32)] * 2,
        input_output_aliases={1: 0},
        compiler_params=pltpu.CompilerParams(vmem_limit_bytes=16 * MIB),
        cost_estimate=priced(4.0),
        name="load",
    )(decay, flow, pressure, *sides)
    return height_rate, potential_rate, velocity_next


def solution(mesh):
    placed = (P("row", "col"), P("row", "col"), P(None, None, "row", "col"))
    return jax.shard_map(
        local,
        mesh=mesh,
        in_specs=placed,
        out_specs=placed,
        check_vma=False,
    )
```
